32 devices in a mesh: groups: 2 (over y), tok: 4 (over z), lat: 2 (over x), rep: 2 (over core).
Axes of the slice: x: 2, y: 2, z: 4, core: 2. Of those that a mesh axis runs over, the one named last changes fastest.
Arguments:
- tokens: bfloat16 [2048, 512], P(('groups', 'tok', 'lat')), parts along dimension 0, may hold values from -15 to 15
- latents: bfloat16 [768, 512], P(('tok', 'lat')), may hold values from -6 to 6
- w_tok: bfloat16 [1, 512, 2, 512], P(None, None, None, 'rep'), may hold values from -1.5 to 1.5
- w_lat: bfloat16 [1, 512, 2, 512], P(None, None, None, 'rep'), may hold values from -1.5 to 1.5
- o_tok: bfloat16 [1, 512, 512], P(None, 'rep'), may hold values from -0.25 to 0.25
- o_lat: bfloat16 [1, 512, 512], P(None, 'rep'), may hold values from -0.25 to 0.25
- g_tok: float32 [1, 512], replicated, may hold values from 0.1 to 1.9
- g_lat: float32 [1, 512], replicated, may hold values from 0.1 to 1.9
Outputs:
- tokens_out: bfloat16 [2048, 512], P(('groups', 'tok', 'lat')), parts along dimension 0
- latents_out: bfloat16 [1536, 512], P(('groups', 'tok', 'lat')), parts along dimension 0
The draws below stay inside these ranges and needn't reach their ends.
There are 2 independent parts, one for each index of `groups`. The reference program is written for one: setup_inputs(seed, part) draws one part's arguments, and reference() takes and returns one part's arrays. A program takes and returns all parts, laid end to end along the dimension named above; an argument that names none is the same for every part. Nothing has to cross between parts.
All inputs are finite; a program needn't handle non-finite values.
Results may differ from the reference program's by a relative error of at most 0.0068.
Values may be sent and summed in bfloat16 or wider, within the bound.
No kernel may reach another device: no remote copies, remote signals or barrier semaphores. Data moves between devices by JAX's collectives and lax.ppermute only.
A program may use at most 64 MiB of HBM per device.

```python
import jax
import jax.numpy as jnp
from jax import lax

D = 512
HEADS = 8
NLAT = 768
LAYERS = 1
TOK_DEV = 128
NTOK = 1024


def projection_draw(key, salt):
    base = jax.random.normal(jax.random.fold_in(key, salt), (LAYERS, D, 2, D), jnp.float32)
    base = jnp.clip(base, -6.0, 6.0) / jnp.sqrt(jnp.float32(D))
    base = jnp.clip(base, -1.5, 1.5)
    return base.astype(jnp.bfloat16)


def draw_w_tok(key, part):
    return projection_draw(key, 21)


def draw_w_lat(key, part):
    return projection_draw(key, 22)


def draw_tokens(key, part):
    noise = jnp.clip(jax.random.normal(jax.random.fold_in(key, 31), (NTOK, D), jnp.float32), -6.0, 6.0)
    values = noise
    return values.astype(jnp.bfloat16)


def levels(rng, extent, shards, least, largest):
    def one(dim, shards_of):
        steps = jax.random.uniform(jax.random.fold_in(jax.random.fold_in(rng, 6), dim), (shards_of,), jnp.float32, least / len(shards), largest / len(shards))
        return jnp.repeat(jnp.exp(steps), extent[dim] // shards_of).reshape((-1,) + (1,) * (len(extent) - dim - 1))

    gain = one(*shards[0])
    for cut in shards[1:]:
        gain = gain * one(*cut)
    return gain


def centred(rng, extent, width, limit, split=(), held_as=jnp.bfloat16):
    values = jax.random.normal(rng, extent, jnp.float32) * width
    if len(split) > 0:
        values = levels(rng, extent, split, -0.22, 0.18) * values
    return jnp.clip(values, min=-limit, max=limit).astype(held_as)


def setup_inputs(seed: int = 0, part: int = 0) -> dict:
    key_of = jax.random.split(jax.random.key(seed), 9)
    part_keys = jax.random.split(jax.random.fold_in(key_of[8], part), 9)
    tokens = draw_tokens(jax.random.fold_in(jax.random.fold_in(key_of[8], part), 71), part)
    latents = centred(key_of[1], (NLAT, D), 1.0, 6.0, ((0, 8),))
    w_tok = draw_w_tok(jax.random.fold_in(key_of[8], 71), part)
    w_lat = draw_w_lat(jax.random.fold_in(key_of[8], 71), part)
    o_tok = centred(key_of[4], (LAYERS, D, D), D ** -0.5, 0.25, ((1, 2),))
    o_lat = centred(key_of[5], (LAYERS, D, D), D ** -0.5, 0.25, ((1, 2),))
    g_tok = jnp.clip(1.0 + 0.18 * jax.random.normal(key_of[6], (LAYERS, D), jnp.float32), 0.1, 1.9)
    g_lat = jnp.clip(1.0 + 0.18 * jax.random.normal(key_of[7], (LAYERS, D), jnp.float32), 0.1, 1.9)
    return {"tokens": tokens, "latents": latents, "w_tok": w_tok, "w_lat": w_lat, "o_tok": o_tok, "o_lat": o_lat, "g_tok": g_tok, "g_lat": g_lat}


EPS = 1e-06

def rms_scale(source, gain_row):
    widened = source.astype(jnp.float32)
    mean_sq = lax.optimization_barrier(jnp.mean(widened * widened, axis=-1, keepdims=True))
    return (widened * lax.rsqrt(mean_sq + EPS) * gain_row).astype(jnp.bfloat16)

def reference(tokens, latents, w_tok, w_lat, o_tok, o_lat, g_tok, g_lat):
    head_size = D // HEADS
    scale = head_size ** (-0.5)
    block_count = NTOK // TOK_DEV
    for layer_index in range(LAYERS):
        tok_in = rms_scale(tokens, g_tok[layer_index])
        lat_in = rms_scale(latents, g_lat[layer_index])
        tok_proj = jnp.dot(tok_in, w_tok[layer_index].reshape(D, 2 * D), preferred_element_type=jnp.float32)
        tok_proj = tok_proj.astype(jnp.bfloat16).reshape(NTOK, 2, HEADS, head_size)
        lat_proj = jnp.dot(lat_in, w_lat[layer_index].reshape(D, 2 * D), preferred_element_type=jnp.float32)
        lat_proj = lat_proj.astype(jnp.bfloat16).reshape(NLAT, 2, HEADS, head_size)
        lat_key = lat_proj[:, 0].astype(jnp.float32)
        lat_val = lat_proj[:, 1].astype(jnp.float32)

        def one_block(block_index):
            block_rows = lax.dynamic_slice_in_dim(tok_proj, (block_index * TOK_DEV).astype(jnp.int32), TOK_DEV, 0)
            tok_key = block_rows[:, 0].astype(jnp.float32)
            tok_val = block_rows[:, 1].astype(jnp.float32)
            scores = jnp.einsum('lhd,thd->hlt', lat_key, tok_key) * scale
            peak_tok = lax.optimization_barrier(jnp.max(scores, axis=1, keepdims=True))
            tok_exp = jnp.exp(scores - peak_tok)
            tok_weights = lax.optimization_barrier((tok_exp / lax.optimization_barrier(jnp.sum(tok_exp, axis=1, keepdims=True))).astype(jnp.bfloat16))
            tok_att = jnp.einsum('hlt,lhd->thd', tok_weights.astype(jnp.float32), lat_val).astype(jnp.bfloat16)
            peak_lat = lax.optimization_barrier(jnp.max(scores, axis=2))
            lat_exp = jnp.exp(scores - peak_lat[:, :, None])
            block_den = lax.optimization_barrier(jnp.sum(lat_exp, axis=2))
            lat_round = lax.optimization_barrier(lat_exp.astype(jnp.bfloat16))
            block_num = jnp.einsum('hlt,thd->lhd', lat_round.astype(jnp.float32), tok_val)
            return (tok_att, block_num, block_den, peak_lat)
        tok_att, block_num, block_den, peaks = lax.map(one_block, jnp.arange(block_count, dtype=jnp.int32))
        score_top = lax.optimization_barrier(jnp.max(peaks, axis=0))
        factor = jnp.exp(peaks - score_top)
        num_total = jnp.einsum('bhl,blhd->lhd', factor, block_num)
        den_total = lax.optimization_barrier(jnp.sum(factor * block_den, axis=0))
        lat_att = (num_total / jnp.transpose(den_total)[:, :, None]).astype(jnp.bfloat16).reshape(NLAT, D)
        tok_att = tok_att.reshape(NTOK, D)
        tok_sum = jnp.dot(tok_att, o_tok[layer_index], preferred_element_type=jnp.float32)
        lat_sum = jnp.dot(lat_att, o_lat[layer_index], preferred_element_type=jnp.float32)
        tokens = (tokens.astype(jnp.float32) + tok_sum).astype(jnp.bfloat16)
        latents = (latents.astype(jnp.float32) + lat_sum).astype(jnp.bfloat16)
    return (tokens, latents)
```

```python
import functools

import jax
import jax.numpy as jnp
from jax import lax
from jax.experimental import pallas as pl
from jax.experimental.pallas import tpu as pltpu
from jax.sharding import PartitionSpec as P

D = 512
HEADS = 8
EPS = 1e-06


def rms_scale(source, gain_row):
    widened = source.astype(jnp.float32)
    mean_sq = jnp.mean(widened * widened, axis=-1, keepdims=True)
    return (widened * lax.rsqrt(mean_sq + EPS) * gain_row).astype(jnp.bfloat16)


def head_terms(per_head):
    tok_key, tok_val, lat_key, lat_val = per_head
    scale = lat_key.shape[1] ** (-0.5)
    scores = (
        lax.dot_general(
            lat_key, tok_key, (((1,), (1,)), ((), ())), preferred_element_type=jnp.float32
        )
        * scale
    )
    peak_tok = jnp.max(scores, axis=0, keepdims=True)
    tok_exp = jnp.exp(scores - peak_tok)
    tok_weights = (tok_exp / jnp.sum(tok_exp, axis=0, keepdims=True)).astype(jnp.bfloat16)
    tok_att = lax.dot_general(
        tok_weights, lat_val, (((0,), (0,)), ((), ())), preferred_element_type=jnp.float32
    )
    peak_lat = jnp.max(scores, axis=1)
    lat_exp = jnp.exp(scores - peak_lat[:, None])
    block_den = jnp.sum(lat_exp, axis=1)
    block_num = jnp.dot(lat_exp.astype(jnp.bfloat16), tok_val, preferred_element_type=jnp.float32)
    return (tok_att.astype(jnp.bfloat16), block_num, block_den, peak_lat)


def wide_body(tokens, latents, w_tok, w_lat, o_tok, o_lat, g_tok, g_lat):
    head_size = D // HEADS
    row_count = tokens.shape[0]
    model_width = tokens.shape[1]
    half_width = w_tok.shape[3]
    head_count = half_width // head_size
    tok_in = rms_scale(tokens, g_tok[0])
    lat_in = rms_scale(latents, g_lat[0])
    tok_proj = jnp.dot(
        tok_in, w_tok[0].reshape(model_width, 2 * half_width), preferred_element_type=jnp.float32
    )
    tok_proj = tok_proj.astype(jnp.bfloat16).reshape(row_count, 2, head_count, head_size)
    lat_own = jnp.dot(
        lat_in, w_lat[0].reshape(model_width, 2 * half_width), preferred_element_type=jnp.float32
    )
    lat_own = lat_own.astype(jnp.bfloat16).reshape(-1, 2, half_width)
    lat_proj = lax.all_gather(lat_own, ("tok", "lat"), axis=0, tiled=True)
    lat_count = lat_proj.shape[0]
    lat_proj = lat_proj.reshape(lat_count, 2, head_count, head_size)
    per_head = (
        jnp.transpose(tok_proj[:, 0], (1, 0, 2)),
        jnp.transpose(tok_proj[:, 1], (1, 0, 2)),
        jnp.transpose(lat_proj[:, 0], (1, 0, 2)),
        jnp.transpose(lat_proj[:, 1], (1, 0, 2)),
    )
    tok_att, block_num, block_den, peaks = lax.map(head_terms, per_head)
    tok_att = jnp.transpose(tok_att, (1, 0, 2)).reshape(row_count, half_width)
    block_num = jnp.transpose(block_num, (1, 0, 2))
    block_den = jnp.transpose(block_den)
    peaks = jnp.transpose(peaks)
    got_num = lax.all_to_all(
        block_num.reshape(lat_count, half_width),
        ("tok", "lat"),
        split_axis=0,
        concat_axis=0,
        tiled=True,
    )
    got_den = lax.all_to_all(block_den, ("tok", "lat"), split_axis=0, concat_axis=0, tiled=True)
    got_peak = lax.all_to_all(peaks, ("tok", "lat"), split_axis=0, concat_axis=0, tiled=True)
    sources = lax.axis_size(("tok", "lat"))
    got_num = got_num.reshape(sources, -1, head_count, head_size)
    got_den = got_den.reshape(sources, -1, head_count)
    got_peak = got_peak.reshape(sources, -1, head_count)
    score_top = jnp.max(got_peak, axis=0)
    factor = jnp.exp(got_peak - score_top)
    num_own = jnp.sum(got_num * factor[:, :, :, None], axis=0)
    den_own = jnp.sum(got_den * factor, axis=0)
    lat_att = (num_own / den_own[:, :, None]).astype(jnp.bfloat16).reshape(-1, half_width)
    lat_part = jnp.dot(lat_att, o_lat[0], preferred_element_type=jnp.float32)
    lat_sum = lax.psum(lat_part, "rep")
    latents = (latents.astype(jnp.float32) + lat_sum).astype(jnp.bfloat16)
    tok_part = jnp.dot(tok_att, o_tok[0], preferred_element_type=jnp.float32)
    tok_sum = lax.psum(tok_part, "rep")
    tokens = (tokens.astype(jnp.float32) + tok_sum).astype(jnp.bfloat16)
    return (tokens, latents)


def attend(query_ref, gain_q, wq_refs, key_refs, gain_k, wkv_refs, o_refs, out_ref, rows_ref):
    head_size = D // HEADS
    half = wq_refs[0].shape[1] // 2
    scale = head_size ** (-0.5)
    queries = query_ref[...]
    query_in = rms_scale(queries, gain_q[...])
    start = 0
    for ref in key_refs:
        rows_ref[start : start + ref.shape[0], :] = rms_scale(ref[...], gain_k[...])
        start += ref.shape[0]
    key_in = rows_ref[0:start, :]
    lanes = 2 * head_size
    lane = lax.broadcasted_iota(jnp.int32, (queries.shape[0], lanes), 1)
    total = queries.astype(jnp.float32)
    for wq, wkv, o_half in zip(wq_refs, wkv_refs, o_refs):
        q = jnp.dot(query_in, wq[:, 0:half], preferred_element_type=jnp.float32) * scale
        kv = jnp.dot(key_in, wkv[...], preferred_element_type=jnp.float32).astype(jnp.bfloat16)
        q = q.astype(jnp.bfloat16)
        for pair in range(half // lanes):
            at = slice(pair * lanes, (pair + 1) * lanes)
            k_pair = kv[:, at]
            v_pair = kv[:, half + pair * lanes : half + (pair + 1) * lanes]
            outs = []
            for head in range(2):
                q_head = jnp.where(lane // head_size == head, q[:, at], jnp.zeros_like(q[:, at]))
                scores = lax.dot_general(
                    q_head, k_pair, (((1,), (1,)), ((), ())), preferred_element_type=jnp.float32
                )
                weights = jnp.exp(scores - jnp.max(scores, axis=1, keepdims=True))
                den = jnp.sum(weights, axis=1, keepdims=True)
                num = jnp.dot(
                    weights.astype(jnp.bfloat16), v_pair, preferred_element_type=jnp.float32
                )
                outs.append(num / den)
            att = jnp.where(lane < head_size, outs[0], outs[1]).astype(jnp.bfloat16)
            total = total + jnp.dot(att, o_half[at, :], preferred_element_type=jnp.float32)
    out_ref[...] = total.astype(jnp.bfloat16)


def attention_kernel(count, core_ref, *refs):
    tok_refs = refs[0:count]
    lat_refs = refs[count : 2 * count]
    wt, wt_far, wl, wl_far, ot, ot_far, ol, ol_far, g_tok, g_lat = refs[2 * count : 2 * count + 10]
    tok_out, lat_out, rows_ref = refs[2 * count + 10 :]
    core = core_ref[0]

    @pl.when(core == 0)
    def _():
        attend(tok_refs[0], g_tok, (wt, wt_far), lat_refs, g_lat, (wl, wl_far), (ot, ot_far), tok_out, rows_ref)

    @pl.when(core != 0)
    def _():
        attend(lat_refs[0], g_lat, (wl, wl_far), tok_refs, g_tok, (wt, wt_far), (ol, ol_far), lat_out, rows_ref)


def near_body(steps, tokens, latents, w_tok, w_lat, o_tok, o_lat, g_tok, g_lat):
    width = tokens.shape[1]
    core = lax.axis_index("rep")
    swap = [(0, 1), (1, 0)]
    axes = ("tok", "lat", "rep")

    def over_tok(rows, step, rep):
        pairs = [
            ((t * 2 + l) * 2 + rep, ((t ^ step) * 2 + l) * 2 + rep)
            for t in range(steps)
            for l in range(2)
        ]
        return lax.ppermute(rows, axes, pairs)

    def over_lat(rows, rep):
        pairs = [
            ((t * 2 + l) * 2 + rep, (t * 2 + 1 - l) * 2 + rep) for t in range(steps) for l in range(2)
        ]
        return lax.ppermute(rows, axes, pairs)

    lat_rows, tok_rows = [latents], [tokens]
    for step in range(steps - 1, 0, -1):
        lat_rows.append(over_tok(latents, step, 0))
        tok_rows.append(over_tok(tokens, step, 1))
    lat_rows += [over_lat(rows, 0) for rows in lat_rows]
    tok_rows += [over_lat(rows, 1) for rows in tok_rows]
    wt_far = lax.ppermute(w_tok, "rep", swap)
    wl_far = lax.ppermute(w_lat, "rep", swap)
    ot_far = lax.ppermute(o_tok, "rep", [(1, 0)])
    ol_far = lax.ppermute(o_lat, "rep", [(0, 1)])
    flat = lambda w: w[0].reshape(width, -1)
    count = len(tok_rows)
    vmem = pl.BlockSpec(memory_space=pltpu.VMEM)
    keys = max(count * tokens.shape[0], count * latents.shape[0])
    tok_new, lat_new = pl.pallas_call(
        functools.partial(attention_kernel, count),
        out_shape=(
            jax.ShapeDtypeStruct(tokens.shape, tokens.dtype),
            jax.ShapeDtypeStruct(latents.shape, latents.dtype),
        ),
        in_specs=[pl.BlockSpec(memory_space=pltpu.SMEM)] + [vmem] * (2 * count + 10),
        out_specs=(vmem, vmem),
        scratch_shapes=[pltpu.VMEM((keys, width), jnp.bfloat16)],
        name="attention",
        compiler_params=pltpu.CompilerParams(vmem_limit_bytes=24 * 1024 * 1024),
    )(
        core.astype(jnp.int32).reshape(1),
        *tok_rows,
        *lat_rows,
        flat(w_tok),
        flat(wt_far),
        flat(w_lat),
        flat(wl_far),
        o_tok[0],
        ot_far[0],
        o_lat[0],
        ol_far[0],
        g_tok,
        g_lat,
    )
    tok_got = lax.ppermute(tok_new, "rep", [(0, 1)])
    lat_got = lax.ppermute(lat_new, "rep", [(1, 0)])
    return jnp.where(core == 0, tok_new, tok_got), jnp.where(core == 0, lat_got, lat_new)


def solution(mesh):
    placed = (
        P(("groups", "tok", "lat"), None),
        P(("tok", "lat"), None),
        P(None, None, None, "rep"),
        P(None, None, None, "rep"),
        P(None, "rep", None),
        P(None, "rep", None),
        P(),
        P(),
    )
    steps = mesh.shape["tok"]
    near = mesh.shape["rep"] == 2 and mesh.shape["lat"] == 2 and steps in (2, 4, 8)
    body = functools.partial(near_body, steps) if near else wide_body
    return jax.shard_map(
        body,
        mesh=mesh,
        in_specs=placed,
        out_specs=(P(("groups", "tok", "lat"), None), P(("groups", "tok", "lat"), None)),
        check_vma=False,
    )
```
